32 devices in a mesh: fsdp: 8 (over y, x, core), dp: 4 (over z).
Axes of the slice: x: 2, y: 2, z: 4, core: 2. Of those that a mesh axis runs over, the one named last changes fastest.
Arguments:
- hidden: bfloat16 [8192, 14336], P(('fsdp', 'dp')), may hold values from -6 to 6
- cotangent: bfloat16 [8192, 4096], P(('fsdp', 'dp')), may hold values from -6 to 6
- tiles: bfloat16 [64, 128, 128], P('fsdp'), may hold values from -0.25 to 0.25
- tile_rows: int32 [64], P('fsdp'), may hold values from 0 to 111, as said below
- tile_cols: int32 [64], P('fsdp'), may hold values from 0 to 31, as said below
- counts: int32 [8], P('fsdp'), may hold values from 1 to 8, as said below
Outputs:
- layer_out: bfloat16 [8192, 4096], P(('fsdp', 'dp'))
- hidden_grad: bfloat16 [8192, 14336], P(('fsdp', 'dp'))
- weight_grad: float32 [64, 128, 128], P('fsdp')
The draws below stay inside these ranges and needn't reach their ends.
Inputs may be any that keep to these rules, and one draw needn't show every extreme that they name: `tile_rows`: every slot (live or not) names a different block; the row block is below 112. `tile_cols`: the column block is below 32. `counts`: some owner has all 8 slots live in every draw.
All inputs are finite; a program needn't handle non-finite values.
Results may differ from the reference program's by a relative error of at most 0.0085.
Values may be sent and summed in bfloat16 or wider, within the bound.
No kernel may reach another device: no remote copies, remote signals or barrier semaphores. Data moves between devices by JAX's collectives and lax.ppermute only.
A program may use at most 192 MiB of HBM per device.

```python
import math
import jax
import jax.numpy as jnp
from jax import lax

D = 4096
FF = 14336
TILE = 128
MAXB = 8
SLOTS = 64
TOKENS = 8192
N_FSDP = 8


def chosen_blocks(key):
    ordering = jax.random.permutation(jax.random.fold_in(key, 11), FF // TILE * (D // TILE))
    picked = ordering[:SLOTS].astype(jnp.int32)
    return jnp.sort(picked).astype(jnp.int32)


def draw_tile_rows(key, part):
    return (chosen_blocks(key) // (D // TILE)).astype(jnp.int32)


def draw_tile_cols(key, part):
    return (chosen_blocks(key) % (D // TILE)).astype(jnp.int32)


def draw_counts(key, part):
    drawn = jax.random.randint(jax.random.fold_in(key, 3), (N_FSDP,), 1, MAXB + 1)
    fullest = jax.random.randint(jax.random.fold_in(key, 5), (), 0, N_FSDP)
    return jnp.where(jnp.arange(N_FSDP) == fullest, MAXB, drawn).astype(jnp.int32)


def draw_hidden(key, part):
    own_key = jax.random.fold_in(key, 21)
    rough_key = jax.random.fold_in(key, 22)
    position = jnp.arange(FF, dtype=jnp.float32) / TILE
    level = jnp.floor(position) / max(FF // TILE - 1, 1)
    rough = jax.random.uniform(rough_key, (FF,), jnp.float32, 0.8, 1.25)
    column_scale = 0.6 * jnp.exp(level * jnp.log(2.0 / 0.6)) * rough
    values = jax.random.truncated_normal(own_key, -2.4, 2.4, (TOKENS, FF), jnp.float32) * column_scale[None, :]
    return values.astype(jnp.bfloat16)


def draw_cotangent(key, part):
    own_key = jax.random.fold_in(key, 23)
    values = jax.random.truncated_normal(own_key, -6.0, 6.0, (TOKENS, D), jnp.float32)
    return values.astype(jnp.bfloat16)


def block_scale(key, dims, cuts, low, high):
    level = 1.0
    for dim, shards_of in cuts:
        draws = jax.random.uniform(jax.random.fold_in(jax.random.fold_in(key, 6), dim), (shards_of,), jnp.float32, low / len(cuts), high / len(cuts))
        level = level * jnp.repeat(jnp.exp(draws), dims[dim] // shards_of).reshape((-1,) + (1,) * (len(dims) - 1 - dim))
    return level


def bell_draw(stream_key, dims, scale, limit, cuts=(), held_as=jnp.bfloat16):
    gain = block_scale(stream_key, dims, cuts, -0.22, 0.18) if cuts else 1.0
    array = jax.random.normal(stream_key, dims, jnp.float32) * scale * gain
    return jnp.minimum(jnp.maximum(array, -limit), limit).astype(held_as)


def setup_inputs(seed: int = 0) -> dict:
    arg_keys = jax.random.split(jax.random.key(seed), 7)
    return {
        "hidden": draw_hidden(jax.random.fold_in(arg_keys[6], 71), 0),
        "cotangent": draw_cotangent(jax.random.fold_in(arg_keys[6], 71), 0),
        "tiles": bell_draw(arg_keys[2], (SLOTS, TILE, TILE), (TILE * MAXB // 2) ** -0.5, 0.25, ((0, 8),)),
        "tile_rows": draw_tile_rows(jax.random.fold_in(arg_keys[6], 71), 0),
        "tile_cols": draw_tile_cols(jax.random.fold_in(arg_keys[6], 71), 0),
        "counts": draw_counts(jax.random.fold_in(arg_keys[6], 71), 0),
    }


def reference(hidden, cotangent, tiles, tile_rows, tile_cols, counts):
    slot_total = tiles.shape[0]
    per_owner = slot_total // N_FSDP
    edge_len = tiles.shape[1]
    slot_index = jnp.arange(slot_total, dtype=jnp.int32)
    live_slots = slot_index % per_owner < counts[slot_index // per_owner]
    masked = jnp.where(live_slots[:, None, None], tiles, jnp.zeros_like(tiles))

    def advance(totals, inputs_now):
        layer_acc, grad_acc = totals
        weight_block, row_id, col_id = inputs_now
        row_at = (row_id * edge_len).astype(jnp.int32)
        col_at = (col_id * edge_len).astype(jnp.int32)
        picked = lax.dynamic_slice_in_dim(hidden, row_at, edge_len, 1)
        upstream = lax.dynamic_slice_in_dim(cotangent, col_at, edge_len, 1)
        forward = jnp.dot(picked, weight_block, preferred_element_type=jnp.float32)
        layer_acc = lax.dynamic_update_slice_in_dim(layer_acc, lax.dynamic_slice_in_dim(layer_acc, col_at, edge_len, 1) + forward, col_at, 1)
        backward = jnp.dot(upstream, weight_block.T, preferred_element_type=jnp.float32)
        grad_acc = lax.dynamic_update_slice_in_dim(grad_acc, lax.dynamic_slice_in_dim(grad_acc, row_at, edge_len, 1) + backward, row_at, 1)
        weight_term = jnp.dot(picked.T, upstream, preferred_element_type=jnp.float32)
        return ((layer_acc, grad_acc), weight_term)
    start_totals = (jnp.zeros(cotangent.shape, jnp.float32), jnp.zeros(hidden.shape, jnp.float32))
    (layer_acc, grad_acc), weight_terms = lax.scan(advance, start_totals, (masked, tile_rows, tile_cols))
    raw_grad = jnp.where(live_slots[:, None, None], weight_terms, jnp.zeros_like(weight_terms))
    squares = jnp.sum(raw_grad * raw_grad)
    entries = jnp.sum(counts).astype(jnp.float32) * edge_len * edge_len
    spread = jnp.sqrt(squares / entries)
    root_tokens = math.sqrt(TOKENS)
    factor = jnp.minimum(1.0, 0.5 * root_tokens / spread) / root_tokens
    return (layer_acc.astype(jnp.bfloat16), grad_acc.astype(jnp.bfloat16), raw_grad * factor)
```

```python
import functools
import math

import jax
import jax.numpy as jnp
from jax import lax
from jax.experimental import pallas as pl
from jax.experimental.pallas import tpu as pltpu
from jax.sharding import PartitionSpec as P


F32, BF16 = jnp.float32, jnp.bfloat16
VMEM = pl.BlockSpec(memory_space=pltpu.VMEM)
SMEM = pl.BlockSpec(memory_space=pltpu.SMEM)
HBM = pl.BlockSpec(memory_space=pltpu.HBM)
UNROLL = 8
CHUNKS = 1


def shaped(dims, dtype):
    return jax.ShapeDtypeStruct(tuple(dims), dtype)


def kernel_call(body, out_shape, in_specs, out_specs, args, scratch=(), grid=(), limit=8, flops=0, moved=1 << 20):
    return pl.pallas_call(
        body,
        out_shape=out_shape,
        grid=grid,
        in_specs=in_specs,
        out_specs=out_specs,
        scratch_shapes=scratch,
        compiler_params=pltpu.CompilerParams(vmem_limit_bytes=limit << 20),
        cost_estimate=pl.CostEstimate(flops=flops, bytes_accessed=moved, transcendentals=0),
    )(*args)


def swap(value, axis, mask):
    size = lax.axis_size(axis)
    return lax.ppermute(value, axis, [(i, i ^ mask) for i in range(size)])


def lanes(block, edge):
    return pl.ds(pl.multiple_of(block * edge, edge), edge)


def contract(left, right, left_dim, right_dim):
    dims = (((left_dim,), (right_dim,)), ((), ()))
    return lax.dot_general(left, right, dims, preferred_element_type=F32)


def stage_kernel(edge, cotangent, flipped):
    def step(i, carry):
        for u in range(UNROLL):
            block = i * UNROLL + u
            flipped[block] = cotangent[:, lanes(block, edge)].T
        return carry

    lax.fori_loop(0, flipped.shape[0] // UNROLL, step, 0)


def terms_kernel(slots, edge, span, flipped, hidden, *refs):
    mine, theirs, where, rows, cols = refs[-5:]
    metas = refs[:-5]
    width = mine.shape[1]
    for parity, target in ((0, mine), (1, theirs)):
        target[...] = jnp.zeros(target.shape, target.dtype)

        end = jnp.int32(0)
        for pair, meta in enumerate(metas):
            for j in span:
                where[end] = pair * width + (j - span[0])
                rows[end] = meta[parity, j]
                cols[end] = meta[parity, slots + j]
                end = end + (j < meta[parity, 2 * slots]).astype(jnp.int32)
        last = jnp.maximum(end - 1, 0)
        for u in range(UNROLL - 1):
            where[end + u] = where[last]
            rows[end + u] = rows[last]
            cols[end + u] = cols[last]

        def step(i, carry):
            for u in range(UNROLL):
                at = i * UNROLL + u
                term = contract(flipped[cols[at]], hidden[:, lanes(rows[at], edge)], 1, 0)
                spot = where[at]
                target[spot // width, spot % width] = term.astype(target.dtype)
            return carry

        lax.fori_loop(0, (end + UNROLL - 1) // UNROLL, step, 0)


def on_chip_kernel(mine, arrived, own, *sent):
    own[...] = mine[0] + arrived[0].astype(F32)
    for m, out in enumerate(sent):
        out[...] = (mine[m + 1] + arrived[m + 1].astype(F32)).astype(BF16)


def in_plane_kernel(share, n_dp, *refs):
    parts, outs = refs[:-n_dp], refs[-n_dp:]
    place = lax.axis_index("dp")
    for m, out in enumerate(outs):
        at = pl.ds((place ^ m) * share, share)
        out[...] = pair_sum([ref[at].astype(F32) for ref in parts]).astype(out.dtype)


def settle_kernel(own, *refs):
    arrived, final, squares = refs[:-2], refs[-2], refs[-1]
    total = pair_sum([own[...]] + [ref[...].astype(F32) for ref in arrived])
    squared = jnp.sum(jnp.sum(total * total, axis=0), axis=0, keepdims=True)
    squares[...] = jnp.broadcast_to(squared, squares.shape)
    for i in range(total.shape[0]):
        final[i] = total[i].T.astype(BF16)


def finish_kernel(root_tokens, slots, edge, chunks, pairs, *refs):
    metas, squares, pieces, out = refs[:pairs], refs[pairs : pairs + chunks], refs[pairs + chunks : -1], refs[-1]
    place = lax.axis_index("dp")
    live = 0
    for meta in metas:
        live = live + meta[0, 2 * slots] + meta[1, 2 * slots]
    entries = live.astype(F32) * (edge * edge)
    total = pair_sum([jnp.sum(ref[...], keepdims=True) for ref in squares])
    spread = jnp.sqrt(total / entries)
    factor = jnp.minimum(1.0, 0.5 * root_tokens / spread) / root_tokens
    per_chunk = len(pieces) // chunks
    for i, piece in enumerate(pieces):
        chunk, m = i // per_chunk, i % per_chunk
        out[chunk * per_chunk + (place ^ m)] = piece[...].astype(F32) * factor[:, :, None]


def products_kernel(slots, edge, out_at, in_at, flip, pairs, source, *refs):
    metas, weights, out = refs[:pairs], refs[pairs : 3 * pairs], refs[3 * pairs]
    held, made, heads, nexts, picks, sources, filled, starts = refs[3 * pairs + 1 :]
    blocks = heads.shape[0] - 1
    group = out.shape[1] // edge

    @pl.when(pl.program_id(0) == 0)
    def _():
        for block in range(blocks):
            heads[block] = -1
        for owner, ref in enumerate(weights):
            held[owner * slots : (owner + 1) * slots] = ref[...]
        at = jnp.int32(0)
        for owner in range(2 * pairs):
            meta, side = metas[owner // 2], owner % 2
            count = meta[side, 2 * slots]
            for j in range(slots):
                block = jnp.where(j < count, meta[side, out_at * slots + j], blocks)
                picks[at] = owner * slots + j
                sources[at] = meta[side, in_at * slots + j]
                nexts[at] = heads[block]
                heads[block] = at
                at = at + (j < count).astype(jnp.int32)
        last = jnp.maximum(at - 1, 0)
        for u in range(UNROLL - 1):
            picks[at + u] = picks[last]
            sources[at + u] = sources[last]

        def step(i, carry):
            for u in range(UNROLL):
                spot = i * UNROLL + u
                left = source[:, lanes(sources[spot], edge)]
                made[spot] = contract(left, held[picks[spot]], 1, 1 if flip else 0)
            return carry

        lax.fori_loop(0, (at + UNROLL - 1) // UNROLL, step, 0)
        at = jnp.int32(0)
        for block in range(blocks):
            if block % group == 0:
                starts[block // group] = at
            filled[at] = block % group
            at = at + (heads[block] >= 0).astype(jnp.int32)
        starts[blocks // group] = at

    turn = pl.program_id(0)
    out[...] = jnp.zeros(out.shape, out.dtype)

    def fill(i, carry):
        first = heads[turn * group + filled[i]]

        def more(s):
            made[first] += made[s]
            return nexts[s]

        lax.while_loop(lambda s: s >= 0, more, nexts[first])
        out[:, lanes(filled[i], edge)] = made[first].astype(out.dtype)
        return carry

    lax.fori_loop(starts[turn], starts[turn + 1], fill, 0)


def products(metas, source, weights, width, slots, edge, flip, steps):
    tokens = source.shape[0]
    blocks = width // edge
    total = len(weights) * slots
    out_at, in_at = (0, 1) if flip else (1, 0)
    return kernel_call(
        functools.partial(products_kernel, slots, edge, out_at, in_at, flip, len(metas)),
        shaped((tokens, width), BF16),
        [VMEM] + [SMEM] * len(metas) + [VMEM] * len(weights),
        pl.BlockSpec((tokens, blocks // steps * edge), lambda i: (0, i)),
        [source] + metas + weights,
        scratch=[
            pltpu.VMEM((total, edge, edge), BF16),
            pltpu.VMEM((total + UNROLL, tokens, edge), F32),
            pltpu.SMEM((blocks + 1,), jnp.int32),
            pltpu.SMEM((total + UNROLL,), jnp.int32),
            pltpu.SMEM((total + UNROLL,), jnp.int32),
            pltpu.SMEM((total + UNROLL,), jnp.int32),
            pltpu.SMEM((blocks + 1,), jnp.int32),
            pltpu.SMEM((steps + 1,), jnp.int32),
        ],
        grid=(steps,),
        limit=24 if total <= 64 else 63,
        flops=1 << 34,
        moved=tokens * width * 2,
    )


def pair_sum(terms):
    while len(terms) > 1:
        terms = [a + b for a, b in zip(terms[::2], terms[1::2])]
    return terms[0]


def shards(hidden, cotangent, tiles, tile_rows, tile_cols, counts):
    n_fsdp, n_dp = lax.axis_size("fsdp"), lax.axis_size("dp")
    tokens = hidden.shape[0]
    slots, edge = tiles.shape[0], tiles.shape[1]
    pairs = n_fsdp // 2
    width = slots // CHUNKS
    share = width // n_dp
    blocks_model = cotangent.shape[1] // edge
    root_tokens = math.sqrt(tokens * n_fsdp * n_dp)
    apart = range(1, pairs)

    filler = jnp.zeros((128 - 2 * slots - 1,), jnp.int32)
    packed = jnp.concatenate([tile_rows, tile_cols, counts, filler])[None]
    near = jnp.concatenate([packed, swap(packed, "fsdp", 1)])
    metas = [near] + [swap(near, "fsdp", 2 * m) for m in apart]

    across = [tiles]
    for m in apart:
        top = 1 << (m.bit_length() - 1)
        across.append(swap(across[m ^ top], "fsdp", 2 * top))
    beside = [swap(across[m], "fsdp", 1) for m in range(pairs)]
    weights = [w for both in zip(across, beside) for w in both]

    flipped = kernel_call(
        functools.partial(stage_kernel, edge),
        shaped((blocks_model, edge, tokens), BF16),
        [VMEM],
        VMEM,
        [cotangent],
        flops=1 << 34,
        moved=4 << 20,
    )

    squares, pieces = [], []
    for c in range(CHUNKS):
        span = range(c * width, (c + 1) * width)
        dims = (pairs, width, edge, edge)
        mine, theirs = kernel_call(
            functools.partial(terms_kernel, slots, edge, span),
            (shaped(dims, F32), shaped(dims, BF16)),
            [VMEM, VMEM] + [SMEM] * pairs,
            (VMEM, VMEM),
            [flipped, hidden] + metas,
            scratch=[pltpu.SMEM((pairs * width + UNROLL,), jnp.int32)] * 3,
            limit=16,
            flops=4 * pairs * width * tokens * edge * edge,
        )
        arrived = swap(theirs, "fsdp", 1)
        own, *sent = kernel_call(
            on_chip_kernel,
            (shaped(dims[1:], F32),) + (shaped(dims[1:], BF16),) * (pairs - 1),
            [VMEM, VMEM],
            (VMEM,) * pairs,
            [mine, arrived],
            flops=1 << 26,
        )
        arrived = [swap(sent[m - 1], "fsdp", 2 * m) for m in apart]
        piece = (share, edge, edge)
        own, *sent = kernel_call(
            functools.partial(in_plane_kernel, share, n_dp),
            (shaped(piece, F32),) + (shaped(piece, BF16),) * (n_dp - 1),
            [VMEM] * pairs,
            (VMEM,) * n_dp,
            [own] + arrived,
            flops=1 << 26,
        )
        arrived = [swap(sent[m - 1], "dp", m) for m in range(1, n_dp)]
        final, squared = kernel_call(
            settle_kernel,
            (shaped(piece, BF16), shaped((n_fsdp * n_dp, edge), F32)),
            [VMEM] * n_dp,
            (VMEM, VMEM),
            [own] + arrived,
            flops=1 << 26,
        )
        pieces += [final] + [swap(final, "dp", m) for m in range(1, n_dp)]
        squares.append(lax.all_to_all(squared, ("fsdp", "dp"), 0, 0, tiled=True))

    hidden_grad = products(metas, cotangent, weights, hidden.shape[1], slots, edge, True, 4)
    layer_out = products(metas, hidden, weights, cotangent.shape[1], slots, edge, False, 2)
    weight_grad = kernel_call(
        functools.partial(finish_kernel, root_tokens, slots, edge, CHUNKS, pairs),
        shaped((CHUNKS * n_dp, share, edge, edge), F32),
        [SMEM] * pairs + [VMEM] * (len(squares) + len(pieces)),
        VMEM,
        metas + squares + pieces,
        flops=1 << 26,
    )
    return layer_out, hidden_grad, weight_grad.reshape(slots, edge, edge)


def solution(mesh):
    placed = (
        P(("fsdp", "dp"), None),
        P(("fsdp", "dp"), None),
        P("fsdp", None, None),
        P("fsdp"),
        P("fsdp"),
        P("fsdp"),
    )
    return jax.shard_map(
        shards,
        mesh=mesh,
        in_specs=placed,
        out_specs=(P(("fsdp", "dp"), None), P(("fsdp", "dp"), None), P("fsdp", None, None)),
        check_vma=False,
    )
```

```python
import functools
import math

import jax
import jax.numpy as jnp
from jax import lax
from jax.experimental import pallas as pl
from jax.experimental.pallas import tpu as pltpu
from jax.sharding import PartitionSpec as P


F32, BF16 = jnp.float32, jnp.bfloat16
VMEM = pl.BlockSpec(memory_space=pltpu.VMEM)
SMEM = pl.BlockSpec(memory_space=pltpu.SMEM)
HBM = pl.BlockSpec(memory_space=pltpu.HBM)
UNROLL = 8
CHUNKS = 1


def shaped(dims, dtype):
    return jax.ShapeDtypeStruct(tuple(dims), dtype)


def kernel_call(body, out_shape, in_specs, out_specs, args, scratch=(), grid=(), limit=8, flops=0, moved=1 << 20):
    return pl.pallas_call(
        body,
        out_shape=out_shape,
        grid=grid,
        in_specs=in_specs,
        out_specs=out_specs,
        scratch_shapes=scratch,
        compiler_params=pltpu.CompilerParams(vmem_limit_bytes=limit << 20),
        cost_estimate=pl.CostEstimate(flops=flops, bytes_accessed=moved, transcendentals=0),
    )(*args)


def swap(value, axis, mask):
    size = lax.axis_size(axis)
    return lax.ppermute(value, axis, [(i, i ^ mask) for i in range(size)])


def turned(m, pairs):
    bits = pairs.bit_length() - 1
    half = bits // 2
    return (m >> half) | ((m & ((1 << half) - 1)) << (bits - half))


def chip_swap(value, m):
    size = lax.axis_size("fsdp")
    masks = (2 * m, 2 * turned(m, size // 2))
    return lax.ppermute(value, "fsdp", [(i, i ^ masks[i & 1]) for i in range(size)])


def lanes(block, edge):
    return pl.ds(pl.multiple_of(block * edge, edge), edge)


def contract(left, right, left_dim, right_dim):
    dims = (((left_dim,), (right_dim,)), ((), ()))
    return lax.dot_general(left, right, dims, preferred_element_type=F32)


def pair_kernel(own, other, out):
    out[0:1] = own[...]
    out[1:2] = other[...]


def stage_kernel(edge, cotangent, flipped):
    def step(i, carry):
        for u in range(UNROLL):
            block = i * UNROLL + u
            flipped[block] = cotangent[:, lanes(block, edge)].T
        return carry

    lax.fori_loop(0, flipped.shape[0] // UNROLL, step, 0)


def terms_kernel(slots, edge, span, flipped, hidden, *refs):
    mine, theirs, where, rows, cols = refs[-5:]
    metas = refs[:-5]
    pairs, width = mine.shape[0], mine.shape[1]
    for parity, target in ((0, mine), (1, theirs)):
        target[...] = jnp.zeros(target.shape, target.dtype)

        end = jnp.int32(0)
        for pair in range(pairs):
            meta = metas[turned(pair, pairs) if parity else pair]
            for j in span:
                where[end] = pair * width + (j - span[0])
                rows[end] = meta[parity, j]
                cols[end] = meta[parity, slots + j]
                end = end + (j < meta[parity, 2 * slots]).astype(jnp.int32)
        last = jnp.maximum(end - 1, 0)
        for u in range(UNROLL - 1):
            where[end + u] = where[last]
            rows[end + u] = rows[last]
            cols[end + u] = cols[last]

        def step(i, carry):
            for u in range(UNROLL):
                at = i * UNROLL + u
                term = contract(flipped[cols[at]], hidden[:, lanes(rows[at], edge)], 1, 0)
                spot = where[at]
                target[spot // width, spot % width] = term.astype(target.dtype)
            return carry

        lax.fori_loop(0, (end + UNROLL - 1) // UNROLL, step, 0)


def fold_kernel(mine, arrived, own, sent):
    half = own.shape[0]
    own[...] = mine[:half] + arrived[:half].astype(F32)
    sent[...] = (mine[half:] + arrived[half:].astype(F32)).astype(BF16)


def in_plane_kernel(share, mine, arrived, *outs):
    place = lax.axis_index("dp")
    for m, out in enumerate(outs):
        at = pl.ds((place ^ m) * share, share)
        out[...] = (mine[0, at] + arrived[0, at].astype(F32)).astype(out.dtype)


def settle_kernel(own, *refs):
    arrived, final, squares = refs[:-2], refs[-2], refs[-1]
    total = pair_sum([own[...]] + [ref[...].astype(F32) for ref in arrived])
    squared = jnp.sum(jnp.sum(total * total, axis=0), axis=0, keepdims=True)
    squares[...] = jnp.broadcast_to(squared[:, None, :], squares.shape)
    for i in range(total.shape[0]):
        final[i] = total[i].T.astype(BF16)


def finish_kernel(root_tokens, slots, edge, chunks, pairs, *refs):
    metas, squares, pieces, out = refs[:pairs], refs[pairs : pairs + chunks], refs[pairs + chunks : -1], refs[-1]
    place = lax.axis_index("dp")
    live = 0
    for meta in metas:
        live = live + meta[0, 2 * slots] + meta[1, 2 * slots]
    entries = live.astype(F32) * (edge * edge)
    total = pair_sum([jnp.sum(ref[:, 0, :], keepdims=True) for ref in squares])
    spread = jnp.sqrt(total / entries)
    factor = jnp.minimum(1.0, 0.5 * root_tokens / spread) / root_tokens
    per_chunk = len(pieces) // chunks
    for i, piece in enumerate(pieces):
        chunk, m = i // per_chunk, i % per_chunk
        out[chunk * per_chunk + (place ^ m)] = piece[...].astype(F32) * factor[:, :, None]


def lists_kernel(slots, plans, *refs):
    metas, lists = refs[:-1], refs[-1]
    pairs = len(metas)
    for plan, (out_at, in_at, blocks, steps) in enumerate(plans):
        picks, sources, nexts, heads, filled, starts = range(6 * plan, 6 * plan + 6)
        for block in range(blocks):
            lists[heads, block] = -1
        at = jnp.int32(0)
        for owner in range(2 * pairs):
            pair, side = owner // 2, owner % 2
            meta = metas[turned(pair, pairs) if side else pair]
            count = meta[side, 2 * slots]
            for j in range(slots):
                block = jnp.where(j < count, meta[side, out_at * slots + j], blocks)
                lists[picks, at] = owner * slots + j
                lists[sources, at] = meta[side, in_at * slots + j]
                lists[nexts, at] = lists[heads, block]
                lists[heads, block] = at
                at = at + (j < count).astype(jnp.int32)
        last = jnp.maximum(at - 1, 0)
        for u in range(UNROLL - 1):
            lists[picks, at + u] = lists[picks, last]
            lists[sources, at + u] = lists[sources, last]
        lists[starts, steps + 1] = at
        group = blocks // steps
        at = jnp.int32(0)
        for block in range(blocks):
            if block % group == 0:
                lists[starts, block // group] = at
            lists[filled, at] = block % group
            at = at + (lists[heads, block] >= 0).astype(jnp.int32)
        lists[starts, steps] = at


def products_kernel(edge, row, steps, flip, lists, source, *refs):
    made, refs = refs[-1], refs[:-1]
    if len(refs) > 2:
        weights, out, held = refs[:-2], refs[-2], refs[-1]
    else:
        weights, (held, out) = (), refs
    picks, sources, nexts, heads, filled, starts = range(row, row + 6)
    group = out.shape[1] // edge

    @pl.when(pl.program_id(0) == 0)
    def _():
        for owner, ref in enumerate(weights):
            count = ref.shape[0]
            held[owner * count : (owner + 1) * count] = ref[...]

        def step(i, carry):
            for u in range(UNROLL):
                spot = i * UNROLL + u
                left = source[:, lanes(lists[sources, spot], edge)]
                made[spot] = contract(left, held[lists[picks, spot]], 1, 1 if flip else 0)
            return carry

        lax.fori_loop(0, (lists[starts, steps + 1] + UNROLL - 1) // UNROLL, step, 0)

    turn = pl.program_id(0)
    out[...] = jnp.zeros(out.shape, out.dtype)

    def fill(i, carry):
        block = lists[filled, i]
        first = lists[heads, turn * group + block]

        def more(s):
            made[first] += made[s]
            return lists[nexts, s]

        lax.while_loop(lambda s: s >= 0, more, lists[nexts, first])
        out[:, lanes(block, edge)] = made[first].astype(out.dtype)
        return carry

    lax.fori_loop(lists[starts, turn], lists[starts, turn + 1], fill, 0)


def products(lists, row, source, weights, width, total, edge, flip, steps):
    tokens = source.shape[0]
    block = pl.BlockSpec((tokens, width // steps), lambda i: (0, i))
    shape, spec = shaped((tokens, width), BF16), block
    if len(weights) > 1:
        shape = (shape, shaped((total, edge, edge), BF16))
        spec = (spec, pl.BlockSpec((total, edge, edge), lambda i: (0, 0, 0)))
    return kernel_call(
        functools.partial(products_kernel, edge, row, steps, flip),
        shape,
        [SMEM] + [VMEM] * (1 + len(weights)),
        spec,
        [lists, source] + weights,
        scratch=[pltpu.VMEM((total + UNROLL, tokens, edge), F32)],
        grid=(steps,),
        limit=24 if total <= 64 else 63,
        flops=1 << 34,
        moved=tokens * width * 2,
    )


def pair_sum(terms):
    while len(terms) > 1:
        terms = [a + b for a, b in zip(terms[::2], terms[1::2])]
    return terms[0]


def shards(hidden, cotangent, tiles, tile_rows, tile_cols, counts):
    n_fsdp, n_dp = lax.axis_size("fsdp"), lax.axis_size("dp")
    tokens = hidden.shape[0]
    slots, edge = tiles.shape[0], tiles.shape[1]
    pairs = n_fsdp // 2
    width = slots // CHUNKS
    share = width // n_dp
    blocks_model = cotangent.shape[1] // edge
    root_tokens = math.sqrt(tokens * n_fsdp * n_dp)
    apart = range(1, pairs)

    filler = jnp.zeros((128 - 2 * slots - 1,), jnp.int32)
    packed = jnp.concatenate([tile_rows, tile_cols, counts, filler])[None]
    near = kernel_call(
        pair_kernel,
        shaped((2, packed.shape[1]), jnp.int32),
        [VMEM, VMEM],
        VMEM,
        [packed, swap(packed, "fsdp", 1)],
        flops=1 << 34,
    )
    metas = [near] + [chip_swap(near, m) for m in apart]

    across = [tiles]
    for m in apart:
        low = m & -m
        across.append(chip_swap(across[m ^ low], low))
    beside = [swap(across[m], "fsdp", 1) for m in range(pairs)]
    weights = [w for both in zip(across, beside) for w in both]

    flipped = kernel_call(
        functools.partial(stage_kernel, edge),
        shaped((blocks_model, edge, tokens), BF16),
        [VMEM],
        VMEM,
        [cotangent],
        flops=1 << 30,
        moved=4 << 20,
    )

    squares, pieces = [], []
    for c in range(CHUNKS):
        span = range(c * width, (c + 1) * width)
        dims = (pairs, width, edge, edge)
        mine, theirs = kernel_call(
            functools.partial(terms_kernel, slots, edge, span),
            (shaped(dims, F32), shaped(dims, BF16)),
            [VMEM, VMEM] + [SMEM] * pairs,
            (VMEM, VMEM),
            [flipped, hidden] + metas,
            scratch=[pltpu.SMEM((pairs * width + UNROLL,), jnp.int32)] * 3,
            limit=16,
            flops=4 * pairs * width * tokens * edge * edge,
        )
        arrived = swap(theirs, "fsdp", 1)
        own, step = mine, 0
        while own.shape[0] > 1:
            half = (own.shape[0] // 2,) + dims[1:]
            own, sent = kernel_call(
                fold_kernel,
                (shaped(half, F32), shaped(half, BF16)),
                [VMEM, VMEM],
                (VMEM, VMEM),
                [own, arrived],
                flops=1 << 33,
                limit=8 if pairs <= 4 else 40,
            )
            arrived = chip_swap(sent, half[0])
            step += 1
        piece = (share, edge, edge)
        own, *sent = kernel_call(
            functools.partial(in_plane_kernel, share),
            (shaped(piece, F32),) + (shaped(piece, BF16),) * (n_dp - 1),
            [VMEM] * 2,
            (VMEM,) * n_dp,
            [own, arrived],
            flops=1 << 33,
        )
        arrived = [swap(sent[m - 1], "dp", m) for m in range(1, n_dp)]
        final, squared = kernel_call(
            settle_kernel,
            (shaped(piece, BF16), shaped((n_fsdp * n_dp, 1, edge), F32)),
            [VMEM] * n_dp,
            (VMEM, VMEM),
            [own] + arrived,
            flops=1 << 33,
        )
        pieces += [final] + [swap(final, "dp", m) for m in range(1, n_dp)]
        squares.append(lax.all_to_all(squared, ("fsdp", "dp"), 0, 0, tiled=True))

    blocks_ff, total = hidden.shape[1] // edge, n_fsdp * slots
    plans = ((1, 0, blocks_model, 2), (0, 1, blocks_ff, 4))
    room = -(-max(total + UNROLL, blocks_ff + 1, blocks_model + 1) // 128) * 128
    lists = kernel_call(
        functools.partial(lists_kernel, slots, plans),
        shaped((6 * len(plans), room), jnp.int32),
        [SMEM] * pairs,
        SMEM,
        metas,
        flops=1 << 30,
    )
    layer_out, held = products(
        lists, 0, hidden, weights, cotangent.shape[1], total, edge, False, plans[0][3]
    )
    hidden_grad = products(
        lists, 6, cotangent, [held], hidden.shape[1], total, edge, True, plans[1][3]
    )
    weight_grad = kernel_call(
        functools.partial(finish_kernel, root_tokens, slots, edge, CHUNKS, pairs),
        shaped((CHUNKS * n_dp, share, edge, edge), F32),
        [SMEM] * pairs + [VMEM] * (len(squares) + len(pieces)),
        VMEM,
        metas + squares + pieces,
        flops=1 << 33,
    )
    return layer_out, hidden_grad, weight_grad.reshape(slots, edge, edge)


def solution(mesh):
    placed = (
        P(("fsdp", "dp"), None),
        P(("fsdp", "dp"), None),
        P("fsdp", None, None),
        P("fsdp"),
        P("fsdp"),
        P("fsdp"),
    )
    return jax.shard_map(
        shards,
        mesh=mesh,
        in_specs=placed,
        out_specs=(P(("fsdp", "dp"), None), P(("fsdp", "dp"), None), P("fsdp", None, None)),
        check_vma=False,
    )
```
